32 devices in a mesh: tm: 8 (over z, y), sym: 4 (over x, core).
Axes of the slice: x: 2, y: 2, z: 4, core: 2. Of those that a mesh axis runs over, the one named last changes fastest.
Arguments:
- trade_age: float32 [65536], P(('tm', 'sym')), may hold values from 0.02 to 20
- trade_size: float32 [65536], P(('tm', 'sym')), may hold values from 0.5 to 4
- owner: int32 [65536, 1], P(('tm', 'sym')), may hold values from 0 to 31; in each aligned block of 2048 rows (0 to 2047, 2048 to 4095, ...) at most 96 rows name the same one
- symbol_lane: int32 [65536], P(('tm', 'sym')), may hold values from 0 to 15
- quote_offset: int32 [65536], P(('tm', 'sym')), may hold values from 0 to 511
- quotes: float32 [64, 4096, 128], P('sym', 'tm'), may hold values from -6 to 6
- rates: float32 [128], replicated, may hold values from 0.05 to 2
Outputs:
- joined: float32 [65536, 128], P(('tm', 'sym'))
The draws below stay inside these ranges and needn't reach their ends.
Inputs may be any that keep to these rules, and one draw needn't show every extreme that they name: Among the 2048 trades of one device no owner is named more than 96 times, and in every draw some device names some owner exactly 96 times. Owner o holds symbols of group o % 4 and quote rows of block o // 4.
All inputs are finite; a program needn't handle non-finite values.
Results may differ from the reference program's by a relative error of at most 0.00002.
Values sent between devices are 32-bit elements; how exact they have to be, the bound alone decides.
A program may use at most 64 MiB of HBM per device.

```python
import math
import jax
import jax.numpy as jnp
import numpy as np

F = 128
TICK_DEV = 2048
SYM_DEV = 16
QT_DEV = 512
TICKS = 65536
SYMS = 64
QT = 4096
CAP = 96
N_SYM = 4
DEVICES = 32


def set_ends(values, own_key, smallest, high):
    extent = values.shape
    index_at = [jax.random.randint(jax.random.fold_in(own_key, axis), (), 0, extent[axis]) for axis in range(len(extent))]
    values = values.at[tuple(index_at)].set(smallest)
    longest = extent.index(max(extent))
    index_at[longest] = (index_at[longest] + 1) % extent[longest]
    return values.at[tuple(index_at)].set(high)


def level_of(stream_key, extent, pieces, low, high):
    factor_of, own = 1.0, jax.random.fold_in(stream_key, 6)
    for dim, shards_of in pieces:
        heights = jnp.exp(jax.random.uniform(jax.random.fold_in(own, dim), (shards_of,), jnp.float32, low / len(pieces), high / len(pieces)))
        factor_of = factor_of * jnp.repeat(heights, extent[dim] // shards_of).reshape([-1 if axis == dim else 1 for axis in range(len(extent))])
    return factor_of


def deal_out(key, own, number, rows, number_of, top, bound, skew):
    sequence = jax.random.permutation(key, number_of)
    heavy_load, ordinary = load_shares(number_of, rows * top, bound, skew, True), load_shares(number_of, rows * top, bound, skew, False)
    places = jnp.arange(number_of)

    def named(sizes, offset_by):
        used = int((sizes > 0).sum())
        fixed = max(1, used // 4)
        shifted = fixed + (places - fixed + offset_by * (used - fixed)) % max(1, number_of - fixed)
        return jnp.zeros((number_of,), jnp.int32).at[sequence[jnp.where(places < fixed, places, shifted)]].set(jnp.asarray(sizes, jnp.int32))

    sizes = jnp.where(number % 4 == 0, named(heavy_load, number // 4), named(ordinary, number - number // 4 - 1))
    mixed = jax.random.permutation(jax.random.fold_in(own, 3), number_of)
    giver, sink = mixed[0:number_of // 2 * 2:2], mixed[1:number_of // 2 * 2:2]
    margin = jnp.minimum(sizes[giver] - 1, bound - sizes[sink]) // 2
    margin = jnp.where((giver == sequence[0]) | (sink == sequence[0]) | (sizes[sink] == 0), 0, jnp.maximum(margin, 0))
    shifted = jax.random.randint(jax.random.fold_in(own, 4), (number_of // 2,), 0, 1 << 20) % (margin + 1)
    sizes = sizes.at[giver].add(-shifted).at[sink].add(shifted)
    labels = jnp.searchsorted(jnp.cumsum(sizes), jnp.arange(rows * top), side="right").astype(jnp.int32)
    listing = labels.reshape(top, rows).T
    listing = listing[jax.random.permutation(jax.random.fold_in(own, 1), rows)]
    offset_by = jax.random.randint(jax.random.fold_in(own, 2), (rows, 1), 0, top)
    return jnp.take_along_axis(listing, (jnp.arange(top)[None, :] + offset_by) % top, axis=1)


def load_shares(amount, total, most, lean, full):
    portions = [(1 << 20) // math.isqrt(rank ** lean) + 1 for rank in range(1, amount + 1)]
    largest = most if full else min(most, max(-(-total // amount), total * portions[0] // sum(portions)))
    least = 1 if total - largest >= amount - 1 else 0
    counts, surplus = [largest] + [least] * (amount - 1), total - largest - least * (amount - 1)
    while surplus > 0:
        free = [i for i in range(1, amount) if counts[i] < largest] or [i for i in range(1, amount) if counts[i] < most]
        mass, budget = sum([portions[i] for i in free]), surplus
        for i in free:
            more = min(most - counts[i], max(1, budget * portions[i] // mass), surplus)
            counts[i] = counts[i] + more
            surplus = surplus - more
    return np.array(counts)


def gaussian(rng, extent, width, most, cuts=(), kind=jnp.bfloat16):
    array = width * jax.random.normal(rng, extent, jnp.float32)
    if cuts:
        array = array * level_of(rng, extent, cuts, -0.22, 0.18)
    return jnp.clip(array, -most, most).astype(kind)


def setup_inputs(seed: int = 0) -> dict:
    arg_keys = jax.random.split(jax.random.key(seed), 8)
    trade_age = jnp.clip(jnp.exp(math.log(20.0) - 6.9077553 * jax.random.uniform(arg_keys[0], (TICKS,), jnp.float32) ** level_of(arg_keys[0], (TICKS,), ((0, 32),), -0.2, 0.2)), 0.02, 20.0)
    trade_size = jnp.clip(jnp.exp(math.log(4.0) - 2.0794415 * jax.random.uniform(arg_keys[1], (TICKS,), jnp.float32) ** level_of(arg_keys[1], (TICKS,), ((0, 32),), -0.2, 0.2)), 0.5, 4.0)
    owner_keys = jax.random.split(jax.random.fold_in(arg_keys[2], 1), TICKS // TICK_DEV)
    owner_turns = jax.random.permutation(jax.random.fold_in(arg_keys[2], 3), TICKS // TICK_DEV)
    owner = jax.vmap(lambda own, number: deal_out(jax.random.fold_in(arg_keys[2], 2), own, number, TICK_DEV, DEVICES, 1, CAP, 2))(owner_keys, owner_turns).reshape((TICKS, 1))
    symbol_lane = set_ends(jax.random.randint(arg_keys[3], (TICKS,), 0, SYM_DEV), jax.random.fold_in(arg_keys[3], 1), 0, SYM_DEV - 1).astype(jnp.int32)
    quote_offset = set_ends(jax.random.randint(arg_keys[4], (TICKS,), 0, QT_DEV), jax.random.fold_in(arg_keys[4], 1), 0, QT_DEV - 1).astype(jnp.int32)
    quotes = gaussian(arg_keys[5], (SYMS, QT, F), 1.0, 6.0, ((0, 4), (1, 8)), jnp.float32)
    rates = jnp.clip(jnp.exp(jax.random.uniform(arg_keys[6], (F,), jnp.float32, math.log(0.05), math.log(2.0))), 0.05, 2.0)
    return {"trade_age": trade_age, "trade_size": trade_size, "owner": owner, "symbol_lane": symbol_lane, "quote_offset": quote_offset, "quotes": quotes, "rates": rates}


def reference(trade_age, trade_size, owner, symbol_lane, quote_offset, quotes, rates):
    target = owner[:, 0]
    symbol = ((target % N_SYM) * SYM_DEV + symbol_lane).astype(jnp.int32)
    quote_row = ((target // N_SYM) * QT_DEV + quote_offset).astype(jnp.int32)
    current = quotes[symbol, quote_row]
    earlier = jnp.maximum(quote_row - 1, 0).astype(jnp.int32)
    previous = jnp.where((quote_row > 0)[:, None], quotes[symbol, earlier], jnp.zeros_like(current))
    weight = jnp.exp(-trade_age[:, None] * rates[None, :])
    return trade_size[:, None] * (weight * current + (1.0 - weight) * previous)
```

```python
import functools

import jax
import jax.numpy as jnp
from jax import lax
from jax.experimental import pallas as pl
from jax.experimental.pallas import tpu as pltpu
from jax.sharding import PartitionSpec as P

LANES = 128
PAD = 8
PLANES = 4
BLOCK = 2048
MESH = pl.DeviceIdType.MESH


def join_kernel(
    cfg,
    owner_hbm, lane_hbm, offset_hbm, age_hbm, rates_hbm, quotes_ref,
    out_ref,
    owner_v, lane_v, offset_v, age_v, rates_v,
    table, recv, sbuf, msg_row, msg_age, got_row, got_age, key_v, cur, prev, bsend, brecv,
    isem, qsem, bsem, rsend, rrecv, asend, arecv, jsend, jrecv, relay,
):
    tm_n, sym_n, cap = cfg
    devices = tm_n * sym_n
    ticks = owner_v.shape[1]
    lane_count, quote_rows, features = quotes_ref.shape
    stride = quote_rows + PAD
    tm, sym = lax.axis_index("tm"), lax.axis_index("sym")
    me = tm * sym_n + sym

    plane_n = devices // PLANES
    bits = plane_n.bit_length() - 1
    z = lax.div(me, plane_n)
    half, quarter = lax.div(z, 2), lax.rem(z, 2)
    inner = lax.rem(half + quarter, 2)
    here = lax.rem(me, plane_n)

    def device(p):
        return (lax.div(p, sym_n), lax.rem(p, sym_n))

    def mate(j):
        q, bit = here, 1
        for _ in range(bits):
            mine = lax.rem(lax.div(here, bit), 2)
            q = q + lax.rem(lax.div(j, bit), 2) * (bit - 2 * bit * mine)
            bit *= 2
        return q

    other = 1 - half
    plane = [z, 2 * half + 1 - quarter, 2 * other + half, 2 * other + other]

    def pick(outer_g, inner_g):
        return plane[outer_g] + inner * (plane[inner_g] - plane[outer_g])

    small = [
        pltpu.make_async_copy(src, dst, isem.at[i])
        for i, (src, dst) in enumerate([
            (owner_hbm, owner_v), (lane_hbm, lane_v), (offset_hbm, offset_v), (age_hbm, age_v),
            (rates_hbm, rates_v),
        ])
    ]
    for copy in small:
        copy.start()

    barrier = pltpu.get_barrier_semaphore()

    def greet(where, first):
        @pl.loop(first, plane_n)
        def _(j):
            pl.semaphore_signal(
                barrier, inc=1, device_id=device(where * plane_n + mate(j)), device_id_type=MESH
            )

    @pl.when(z > 0)
    def _():
        greet(z - 1, 0)

    @pl.when(z < PLANES - 1)
    def _():
        greet(z + 1, 0)

    greet(z, 1)

    loads = [
        pltpu.make_async_copy(
            quotes_ref.at[lane], table.at[pl.ds(lane * stride + PAD, quote_rows)], qsem.at[lane]
        )
        for lane in range(lane_count)
    ]
    for load in loads:
        load.start()
    for copy in small:
        copy.wait()

    owner = owner_v[...]
    mine = owner == lax.broadcasted_iota(jnp.int32, (devices, ticks), 0)
    hot = mine.astype(jnp.float32)
    hot_b = hot.astype(jnp.bfloat16)
    width = 256 if ticks % 256 == 0 else 128
    upper = (
        lax.broadcasted_iota(jnp.int32, (width, width), 0)
        < lax.broadcasted_iota(jnp.int32, (width, width), 1)
    ).astype(jnp.float32).astype(jnp.bfloat16)
    base = jnp.zeros((devices, 1), jnp.float32)
    ranks = []
    for start in range(0, ticks, width):
        part = hot[:, start:start + width]
        before = jnp.dot(
            hot_b[:, start:start + width], upper, preferred_element_type=jnp.float32
        )
        ranks.append(jnp.sum(part * (before + base), axis=0, keepdims=True))
        base = base + jnp.sum(part, axis=1, keepdims=True)
    rank = jnp.concatenate(ranks, axis=1).astype(jnp.int32)
    key = owner * LANES + jnp.clip(rank, 0, cap - 1)

    place = (
        rank == lax.broadcasted_iota(jnp.int32, (LANES, ticks), 0)
    ).astype(jnp.float32).astype(jnp.bfloat16)
    local = lane_v[...] * stride + PAD - 1 + offset_v[...]
    age = age_v[...]
    high = age.astype(jnp.bfloat16).astype(jnp.float32)
    middle = (age - high).astype(jnp.bfloat16).astype(jnp.float32)
    low = age - high - middle
    pieces = [
        (local // LANES).astype(jnp.float32), (local % LANES).astype(jnp.float32), high, middle, low
    ]
    spread = jnp.concatenate([(hot * piece).astype(jnp.bfloat16) for piece in pieces], axis=0)
    put = lax.dot_general(
        spread, place, (((1,), (1,)), ((), ())), preferred_element_type=jnp.float32
    )
    taken = [put[i * devices:(i + 1) * devices] for i in range(5)]
    msg_row[:, 0, :] = jnp.clip(
        (taken[0] * LANES + taken[1]).astype(jnp.int32), PAD - 1, lane_count * stride - 2
    )
    msg_age[:, 0, :] = (taken[2] + taken[3]) + taken[4]

    def row_message(p, slot):
        return pltpu.make_async_remote_copy(
            src_ref=msg_row.at[p], dst_ref=got_row.at[slot],
            send_sem=rsend.at[p], recv_sem=rrecv.at[slot],
            device_id=device(p), device_id_type=MESH,
        )

    def age_message(p, slot):
        return pltpu.make_async_remote_copy(
            src_ref=msg_age.at[p], dst_ref=got_age.at[slot],
            send_sem=asend.at[p], recv_sem=arecv.at[slot],
            device_id=device(p), device_id_type=MESH,
        )

    def ask(where, first):
        @pl.loop(first, plane_n)
        def _(j):
            p = where * plane_n + mate(j)
            row_message(p, me).start()
            age_message(p, me).start()

    def boundary():
        return pltpu.make_async_remote_copy(
            src_ref=bsend, dst_ref=brecv, send_sem=bsem.at[0], recv_sem=bsem.at[1],
            device_id=(lax.rem(tm + 1, tm_n), sym), device_id_type=MESH,
        )

    for load in loads:
        load.wait()
    for lane in range(lane_count):
        bsend[lane:lane + 1, :] = table[(lane + 1) * stride - 1:(lane + 1) * stride, :]

    pl.semaphore_wait(barrier, plane_n - 1 + plane_n + plane_n * inner)

    def tell(where, which):
        pl.semaphore_signal(
            relay.at[which], inc=1, device_id=device(where * plane_n + here), device_id_type=MESH
        )

    @pl.when(inner == 1)
    def _():
        tell(z - 1, 0)
        tell(z + 1, 0)

    @pl.when(tm < tm_n - 1)
    def _():
        boundary().start()

    @pl.when(z > 0)
    def _():
        ask(z - 1, 0)

    @pl.when(z < PLANES - 1)
    def _():
        ask(z + 1, 0)

    ask(z, 1)

    pl.semaphore_wait(relay.at[0], 1)

    @pl.when(inner == 1)
    def _():
        tell(3 * half, 1)

    ask(z + 2 - 4 * half, 0)

    @pl.when(inner == 0)
    def _():
        pl.semaphore_wait(relay.at[1], 1)
        ask(3 - z, 0)

    own_row = pltpu.make_async_copy(msg_row.at[me], got_row.at[me], isem.at[0])
    own_row.start()

    @pl.when(tm == 0)
    def _():
        brecv[...] = jnp.zeros_like(brecv)

    @pl.when(tm > 0)
    def _():
        boundary().wait_recv()

    edge = brecv[...]
    for lane in range(lane_count):
        table[lane * stride + PAD - 1:lane * stride + PAD, :] = edge[lane:lane + 1, :]

    rates = rates_v[...]

    def joined(p, ages):
        for r in range(cap):
            row = got_row[p, 0, r]
            cur[r:r + 1, :] = table[pl.ds(row + 1, 1), :]
            prev[r:r + 1, :] = table[pl.ds(row, 1), :]
        ages = jnp.transpose(jnp.broadcast_to(ages, (LANES, LANES)))[:cap]
        weight = jnp.exp(-ages * rates)
        return weight * cur[...] + (1.0 - weight) * prev[...]

    def share(p, source):
        return pltpu.make_async_remote_copy(
            src_ref=sbuf.at[p], dst_ref=recv.at[source, pl.ds(0, cap)],
            send_sem=jsend.at[p], recv_sem=jrecv.at[source],
            device_id=device(p), device_id_type=MESH,
        )

    def serve(where, first, last):
        @pl.loop(first, last)
        def _(j):
            p = where * plane_n + mate(j)
            row_message(p, p).wait_recv()
            age_message(p, p).wait_recv()
            sbuf[p] = joined(p, got_age[p])
            share(p, me).start()

    few = plane_n // 4
    serve(pick(1, 2), 0, few)
    serve(pick(2, 3), 0, plane_n)
    serve(pick(1, 2), few, plane_n)
    serve(pick(3, 1), 0, plane_n)
    serve(z, 1, plane_n)

    own_row.wait()
    recv[me, 0:cap, :] = joined(me, msg_age[me])
    if cap < LANES:
        @pl.loop(0, devices)
        def _(p):
            recv[p, cap:, :] = jnp.zeros((LANES - cap, features), jnp.float32)

    for start in range(0, ticks, LANES):
        key_v[start:start + LANES, :] = jnp.transpose(
            jnp.broadcast_to(key[:, start:start + LANES], (LANES, LANES))
        )

    block = BLOCK if ticks % BLOCK == 0 else LANES
    slots = lax.broadcasted_iota(jnp.int32, (1, LANES), 1)

    def absorb(pa, pb, fresh):
        both = jnp.concatenate([recv[pa], recv[pb]], axis=0)
        first = both.astype(jnp.bfloat16)
        second = (both - first.astype(jnp.float32)).astype(jnp.bfloat16)
        parts = jnp.concatenate([first, second], axis=1)
        slot_a, slot_b = pa * LANES + slots, pb * LANES + slots

        @pl.loop(0, ticks // block)
        def _(b):
            rows = pl.ds(pl.multiple_of(b * block, block), block)
            keys = key_v[rows, :]
            chosen = jnp.concatenate([
                (keys == slot_a).astype(jnp.float32).astype(jnp.bfloat16),
                (keys == slot_b).astype(jnp.float32).astype(jnp.bfloat16),
            ], axis=1)
            got = jnp.dot(chosen, parts, preferred_element_type=jnp.float32)
            got = got[:, :features] + got[:, features:]
            out_ref[rows, :] = got if fresh else out_ref[rows, :] + got

    def arrived(p):
        share(p, p).wait_recv()

    partner = z * plane_n + mate(1)
    arrived(partner)
    absorb(me, partner, True)

    for where, first in (
        (z, 1), (plane[1], 0), (pick(2, 3), 0), (pick(3, 2), 0),
    ):
        @pl.loop(first, plane_n // 2)
        def _(i, where=where):
            pa = where * plane_n + mate(2 * i)
            pb = where * plane_n + mate(2 * i + 1)
            arrived(pa)
            arrived(pb)
            absorb(pa, pb, False)

    @pl.when(tm < tm_n - 1)
    def _():
        boundary().wait_send()

    def settle(where, first):
        @pl.loop(first, plane_n)
        def _(j):
            p = where * plane_n + mate(j)
            row_message(p, me).wait_send()
            age_message(p, me).wait_send()
            share(p, me).wait_send()

    settle(z, 1)
    for where in plane[1:]:
        settle(where, 0)


def per_device(trade_age, trade_size, owner, symbol_lane, quote_offset, quotes, rates):
    tm_n, sym_n = lax.axis_size("tm"), lax.axis_size("sym")
    devices = tm_n * sym_n
    ticks = trade_age.shape[0]
    cap = 3 * ticks // (2 * devices)
    lane_count, quote_rows, features = quotes.shape
    dma = pltpu.SemaphoreType.DMA
    operands = [
        pltpu.with_memory_space_constraint(x, pltpu.HBM)
        for x in (
            owner.reshape(1, ticks), symbol_lane.reshape(1, ticks),
            quote_offset.reshape(1, ticks), trade_age.reshape(1, ticks),
            rates.reshape(1, features), quotes,
        )
    ]
    joined = pl.pallas_call(
        functools.partial(join_kernel, (tm_n, sym_n, cap)),
        out_shape=jax.ShapeDtypeStruct((ticks, features), jnp.float32),
        in_specs=[pl.BlockSpec(memory_space=pltpu.HBM)] * 6,
        out_specs=pl.BlockSpec(memory_space=pltpu.VMEM),
        scratch_shapes=[
            pltpu.VMEM((1, ticks), jnp.int32),
            pltpu.VMEM((1, ticks), jnp.int32),
            pltpu.VMEM((1, ticks), jnp.int32),
            pltpu.VMEM((1, ticks), jnp.float32),
            pltpu.VMEM((1, features), jnp.float32),
            pltpu.VMEM((lane_count * (quote_rows + PAD), features), jnp.float32),
            pltpu.VMEM((devices, LANES, features), jnp.float32),
            pltpu.VMEM((devices, cap, features), jnp.float32),
            pltpu.VMEM((devices, 1, LANES), jnp.int32),
            pltpu.VMEM((devices, 1, LANES), jnp.float32),
            pltpu.SMEM((devices, 1, LANES), jnp.int32),
            pltpu.VMEM((devices, 1, LANES), jnp.float32),
            pltpu.VMEM((ticks, LANES), jnp.int32),
            pltpu.VMEM((cap, features), jnp.float32),
            pltpu.VMEM((cap, features), jnp.float32),
            pltpu.VMEM((lane_count, features), jnp.float32),
            pltpu.VMEM((lane_count, features), jnp.float32),
            dma((5,)), dma((lane_count,)), dma((2,)),
            dma((devices,)), dma((devices,)), dma((devices,)), dma((devices,)),
            dma((devices,)), dma((devices,)),
            pltpu.SemaphoreType.REGULAR((2,)),
        ],
        compiler_params=pltpu.CompilerParams(
            collective_id=0, has_side_effects=True, vmem_limit_bytes=32 << 20
        ),
    )(*operands)
    return trade_size[:, None] * joined


def solution(mesh):
    in_specs = (
        P(("tm", "sym")),
        P(("tm", "sym")),
        P(("tm", "sym"), None),
        P(("tm", "sym")),
        P(("tm", "sym")),
        P("sym", "tm", None),
        P(),
    )
    out_specs = P(("tm", "sym"), None)
    return jax.shard_map(
        per_device, mesh=mesh, in_specs=in_specs, out_specs=out_specs, check_vma=False
    )
```

```python
import functools

import jax
import jax.numpy as jnp
from jax import lax
from jax.experimental import pallas as pl
from jax.experimental.pallas import tpu as pltpu
from jax.sharding import PartitionSpec as P

LANES = 128
PAD = 8
PLANES = 4
BLOCK = 2048
MESH = pl.DeviceIdType.MESH


def join_kernel(
    cfg,
    owner_hbm, lane_hbm, offset_hbm, age_hbm, size_hbm, rates_hbm, quotes_ref,
    out_ref,
    owner_v, lane_v, offset_v, age_v, size_v, rates_v,
    table, recv, sbuf, msg_row, msg_age, got_row, got_age, key_v, scale_v, cur, prev, bsend, brecv, tail,
    isem, qsem, bsem, rsend, rrecv, asend, arecv, jsend, jrecv, relay,
):
    tm_n, sym_n, cap = cfg
    devices = tm_n * sym_n
    ticks = owner_v.shape[1]
    lane_count, quote_rows, features = quotes_ref.shape
    stride = quote_rows + PAD
    tm, sym = lax.axis_index("tm"), lax.axis_index("sym")
    me = tm * sym_n + sym

    plane_n = devices // PLANES
    bits = plane_n.bit_length() - 1
    z = lax.div(me, plane_n)
    half, quarter = lax.div(z, 2), lax.rem(z, 2)
    inner = lax.rem(half + quarter, 2)
    here = lax.rem(me, plane_n)

    def device(p):
        return (lax.div(p, sym_n), lax.rem(p, sym_n))

    flip = [(1 << i) - (2 << i) * lax.rem(lax.div(here, 1 << i), 2) for i in range(bits)]

    def mate(j):
        q = here
        for i, step in enumerate(flip):
            if not isinstance(j, int):
                q = q + lax.rem(lax.div(j, 1 << i), 2) * step
            elif j >> i & 1:
                q = q + step
        return q

    other = 1 - half
    plane = [z, 2 * half + 1 - quarter, 2 * other + half, 2 * other + other]

    def pick(outer_g, inner_g):
        return plane[outer_g] + inner * (plane[inner_g] - plane[outer_g])

    small = [
        pltpu.make_async_copy(src, dst, isem.at[i])
        for i, (src, dst) in enumerate([
            (owner_hbm, owner_v), (lane_hbm, lane_v), (offset_hbm, offset_v), (age_hbm, age_v),
            (rates_hbm, rates_v), (size_hbm, size_v),
        ])
    ]
    last_rows = pltpu.make_async_copy(
        quotes_ref.at[:, pl.ds(quote_rows - PAD, PAD)], tail, isem.at[6]
    )
    for copy in small:
        copy.start()
    last_rows.start()

    barrier = pltpu.get_barrier_semaphore()

    def greet(p):
        pl.semaphore_signal(barrier, inc=1, device_id=device(p), device_id_type=MESH)

    rows_n = tm_n // PLANES
    first_row = 1 - lax.div(lax.rem(tm, rows_n) + rows_n - 1, rows_n)
    last_row = lax.div(lax.rem(tm, rows_n) + 1, rows_n)

    @pl.when(inner == 1)
    def _():
        for j in range(plane_n):
            greet(plane[2] * plane_n + mate(j))
        for j in range(plane_n):
            greet(plane[1] * plane_n + mate(j))

    @pl.when(inner == 0)
    def _():
        greet(plane[1] * plane_n + here)

    for j in range(plane_n - 1, 0, -1):
        greet(z * plane_n + mate(j))

    loads = [
        pltpu.make_async_copy(
            quotes_ref.at[lane], table.at[pl.ds(lane * stride + PAD, quote_rows)], qsem.at[lane]
        )
        for lane in range(lane_count)
    ]
    for load in loads:
        load.start()
    for copy in small:
        copy.wait()

    owner = owner_v[...]
    mine = owner == lax.broadcasted_iota(jnp.int32, (devices, ticks), 0)
    hot = mine.astype(jnp.float32)
    hot_b = hot.astype(jnp.bfloat16)
    width = 256 if ticks % 256 == 0 else 128
    upper = (
        lax.broadcasted_iota(jnp.int32, (width, width), 0)
        < lax.broadcasted_iota(jnp.int32, (width, width), 1)
    ).astype(jnp.float32).astype(jnp.bfloat16)
    base = jnp.zeros((devices, 1), jnp.float32)
    ranks = []
    for start in range(0, ticks, width):
        part = hot[:, start:start + width]
        before = jnp.dot(
            hot_b[:, start:start + width], upper, preferred_element_type=jnp.float32
        )
        ranks.append(jnp.sum(part * (before + base), axis=0, keepdims=True))
        base = base + jnp.sum(part, axis=1, keepdims=True)
    rank = jnp.concatenate(ranks, axis=1).astype(jnp.int32)
    key = owner * LANES + jnp.clip(rank, 0, cap - 1)

    place = (
        rank == lax.broadcasted_iota(jnp.int32, (LANES, ticks), 0)
    ).astype(jnp.float32).astype(jnp.bfloat16)
    local = lane_v[...] * stride + PAD - 1 + offset_v[...]
    age = age_v[...]
    high = age.astype(jnp.bfloat16).astype(jnp.float32)
    middle = (age - high).astype(jnp.bfloat16).astype(jnp.float32)
    low = age - high - middle
    pieces = [
        (local // LANES).astype(jnp.float32), (local % LANES).astype(jnp.float32), high, middle, low
    ]
    spread = jnp.concatenate([(hot * piece).astype(jnp.bfloat16) for piece in pieces], axis=0)
    put = lax.dot_general(
        spread, place, (((1,), (1,)), ((), ())), preferred_element_type=jnp.float32
    )
    taken = [put[i * devices:(i + 1) * devices] for i in range(5)]
    msg_row[:, 0, :] = jnp.clip(
        (taken[0] * LANES + taken[1]).astype(jnp.int32), PAD - 1, lane_count * stride - 2
    )
    msg_age[:, 0, :] = (taken[2] + taken[3]) + taken[4]

    def row_message(p, slot):
        return pltpu.make_async_remote_copy(
            src_ref=msg_row.at[p], dst_ref=got_row.at[slot],
            send_sem=rsend, recv_sem=rrecv.at[slot],
            device_id=device(p), device_id_type=MESH,
        )

    def age_message(p, slot):
        return pltpu.make_async_remote_copy(
            src_ref=msg_age.at[p], dst_ref=got_age.at[slot],
            send_sem=asend, recv_sem=arecv.at[slot],
            device_id=device(p), device_id_type=MESH,
        )

    def ask(where, first, last):
        for j in range(first, last):
            p = where * plane_n + mate(j)
            row_message(p, me).start()
            age_message(p, me).start()

    def boundary():
        return pltpu.make_async_remote_copy(
            src_ref=bsend, dst_ref=brecv, send_sem=bsem.at[0], recv_sem=bsem.at[1],
            device_id=(lax.rem(tm + 1, tm_n), sym), device_id_type=MESH,
        )

    last_rows.wait()
    for lane in range(lane_count):
        bsend[lane:lane + 1, :] = tail[lane, PAD - 1:PAD, :]

    def tell(where, which):
        pl.semaphore_signal(
            relay.at[which], inc=1, device_id=device(where * plane_n + here), device_id_type=MESH
        )

    def heard(which):
        pl.semaphore_wait(relay.at[which], 1)

    near = pick(1, 2)

    pl.semaphore_wait(barrier, 2 * plane_n - 1 + inner)

    @pl.when(last_row * half == 0)
    def _():
        boundary().start()

    ask(near, 0, plane_n)

    @pl.when(inner == 1)
    def _():
        tell(plane[1], 1)
        heard(1)
        tell(plane[2], 2)

        @pl.when(last_row * half == 1)
        def _():
            boundary().start()

        ask(plane[1], 0, plane_n)
        heard(2)
        tell(plane[1], 2)
        ask(plane[3], 0, plane_n)

    @pl.when(inner == 0)
    def _():
        tell(plane[1], 1)
        heard(1)
        ask(plane[2], 0, plane_n)
        heard(2)
        ask(plane[3], 0, plane_n)

    ask(z, 1, plane_n)

    own_row = pltpu.make_async_copy(msg_row.at[me], got_row.at[me], isem.at[0])
    own_row.start()

    @pl.when(tm == 0)
    def _():
        brecv[...] = jnp.zeros_like(brecv)

    @pl.when(tm > 0)
    def _():
        boundary().wait_recv()

    for load in loads:
        load.wait()
    edge = brecv[...]
    for lane in range(lane_count):
        table[lane * stride + PAD - 1:lane * stride + PAD, :] = edge[lane:lane + 1, :]

    rates = rates_v[...]

    def joined(p, ages):
        for r in range(cap):
            row = got_row[p, 0, r]
            cur[r:r + 1, :] = table[pl.ds(row + 1, 1), :]
            prev[r:r + 1, :] = table[pl.ds(row, 1), :]
        ages = jnp.transpose(jnp.broadcast_to(ages, (LANES, LANES)))[:cap]
        weight = jnp.exp(-ages * rates)
        return weight * cur[...] + (1.0 - weight) * prev[...]

    def share(p, source):
        return pltpu.make_async_remote_copy(
            src_ref=sbuf.at[p], dst_ref=recv.at[source, pl.ds(0, cap)],
            send_sem=jsend, recv_sem=jrecv.at[source],
            device_id=device(p), device_id_type=MESH,
        )

    def sent(src, dst, sem):
        pltpu.make_async_remote_copy(
            src_ref=src.at[pl.ds(0, devices - 1)], dst_ref=dst, send_sem=sem,
            recv_sem=jrecv.at[0], device_id=device(z * plane_n + mate(1)), device_id_type=MESH,
        ).wait_send()

    def serve(where, first, last):
        @pl.loop(first, last)
        def _(j):
            p = where * plane_n + mate(j)
            row_message(p, p).wait_recv()
            age_message(p, p).wait_recv()
            sbuf[p] = joined(p, got_age[p])
            share(p, me).start()

    few = plane_n // 4
    serve(pick(1, 2), 0, few)
    serve(pick(2, 3), 0, plane_n)
    serve(pick(1, 2), few, plane_n)
    serve(pick(3, 1), 0, plane_n)
    serve(z, 1, plane_n)

    sent(msg_row, got_row.at[pl.ds(0, devices - 1)], rsend)
    sent(msg_age, got_age.at[pl.ds(0, devices - 1)], asend)
    own_row.wait()
    recv[me, 0:cap, :] = joined(me, msg_age[me])
    if cap < LANES:
        @pl.loop(0, devices)
        def _(p):
            recv[p, cap:, :] = jnp.zeros((LANES - cap, features), jnp.float32)

    for start in range(0, ticks, LANES):
        key_v[start:start + LANES, :] = jnp.transpose(
            jnp.broadcast_to(key[:, start:start + LANES], (LANES, LANES))
        )
        scale_v[start:start + LANES, :] = jnp.transpose(
            jnp.broadcast_to(size_v[:, start:start + LANES], (LANES, LANES))
        )

    block = BLOCK if ticks % BLOCK == 0 else LANES
    slots = lax.broadcasted_iota(jnp.int32, (1, LANES), 1)

    def absorb(pa, pb, fresh=False, final=False):
        both = jnp.concatenate([recv[pa], recv[pb]], axis=0)
        first = both.astype(jnp.bfloat16)
        second = (both - first.astype(jnp.float32)).astype(jnp.bfloat16)
        parts = jnp.concatenate([first, second], axis=1)
        slot_a, slot_b = pa * LANES + slots, pb * LANES + slots

        @pl.loop(0, ticks // block)
        def _(b):
            rows = pl.ds(pl.multiple_of(b * block, block), block)
            keys = key_v[rows, :]
            chosen = jnp.concatenate([
                (keys == slot_a).astype(jnp.float32).astype(jnp.bfloat16),
                (keys == slot_b).astype(jnp.float32).astype(jnp.bfloat16),
            ], axis=1)
            got = jnp.dot(chosen, parts, preferred_element_type=jnp.float32)
            got = got[:, :features] + got[:, features:]
            if not fresh:
                got = out_ref[rows, :] + got
            out_ref[rows, :] = got * scale_v[rows, :] if final else got

    def arrived(p):
        share(p, p).wait_recv()

    partner = z * plane_n + mate(1)
    arrived(partner)
    absorb(me, partner, fresh=True)

    def collect(where, i, final=False):
        pa = where * plane_n + mate(2 * i)
        pb = where * plane_n + mate(2 * i + 1)
        arrived(pa)
        arrived(pb)
        absorb(pa, pb, final=final)

    pairs = plane_n // 2
    last = pick(3, 2)
    for where, first, stop in (
        (z, 1, pairs), (plane[1], 0, pairs), (pick(2, 3), 0, pairs), (last, 0, pairs - 1),
    ):
        @pl.loop(first, stop)
        def _(i, where=where):
            collect(where, i)

    collect(last, pairs - 1, True)

    @pl.when(tm < tm_n - 1)
    def _():
        boundary().wait_send()

    sent(sbuf, recv.at[pl.ds(0, devices - 1), pl.ds(0, cap)], jsend)


def per_device(trade_age, trade_size, owner, symbol_lane, quote_offset, quotes, rates):
    tm_n, sym_n = lax.axis_size("tm"), lax.axis_size("sym")
    devices = tm_n * sym_n
    ticks = trade_age.shape[0]
    cap = 3 * ticks // (2 * devices)
    lane_count, quote_rows, features = quotes.shape
    dma = pltpu.SemaphoreType.DMA
    operands = [
        pltpu.with_memory_space_constraint(x, pltpu.HBM)
        for x in (
            owner.reshape(1, ticks), symbol_lane.reshape(1, ticks),
            quote_offset.reshape(1, ticks), trade_age.reshape(1, ticks),
            trade_size.reshape(1, ticks),
            rates.reshape(1, features), quotes,
        )
    ]
    joined = pl.pallas_call(
        functools.partial(join_kernel, (tm_n, sym_n, cap)),
        out_shape=jax.ShapeDtypeStruct((ticks, features), jnp.float32),
        in_specs=[pl.BlockSpec(memory_space=pltpu.HBM)] * 7,
        out_specs=pl.BlockSpec(memory_space=pltpu.VMEM),
        scratch_shapes=[
            pltpu.VMEM((1, ticks), jnp.int32),
            pltpu.VMEM((1, ticks), jnp.int32),
            pltpu.VMEM((1, ticks), jnp.int32),
            pltpu.VMEM((1, ticks), jnp.float32),
            pltpu.VMEM((1, ticks), jnp.float32),
            pltpu.VMEM((1, features), jnp.float32),
            pltpu.VMEM((lane_count * (quote_rows + PAD), features), jnp.float32),
            pltpu.VMEM((devices, LANES, features), jnp.float32),
            pltpu.VMEM((devices, cap, features), jnp.float32),
            pltpu.VMEM((devices, 1, LANES), jnp.int32),
            pltpu.VMEM((devices, 1, LANES), jnp.float32),
            pltpu.SMEM((devices, 1, LANES), jnp.int32),
            pltpu.VMEM((devices, 1, LANES), jnp.float32),
            pltpu.VMEM((ticks, LANES), jnp.int32),
            pltpu.VMEM((ticks, features), jnp.float32),
            pltpu.VMEM((cap, features), jnp.float32),
            pltpu.VMEM((cap, features), jnp.float32),
            pltpu.VMEM((lane_count, features), jnp.float32),
            pltpu.VMEM((lane_count, features), jnp.float32),
            pltpu.VMEM((lane_count, PAD, features), jnp.float32),
            dma((7,)), dma((lane_count,)), dma((2,)),
            dma, dma((devices,)), dma, dma((devices,)), dma, dma((devices,)),
            pltpu.SemaphoreType.REGULAR((3,)),
        ],
        compiler_params=pltpu.CompilerParams(
            collective_id=0, has_side_effects=True, vmem_limit_bytes=32 << 20
        ),
    )(*operands)
    return joined


def solution(mesh):
    in_specs = (
        P(("tm", "sym")),
        P(("tm", "sym")),
        P(("tm", "sym"), None),
        P(("tm", "sym")),
        P(("tm", "sym")),
        P("sym", "tm", None),
        P(),
    )
    out_specs = P(("tm", "sym"), None)
    return jax.shard_map(
        per_device, mesh=mesh, in_specs=in_specs, out_specs=out_specs, check_vma=False
    )
```

```python
import functools

import jax
import jax.numpy as jnp
from jax import lax
from jax.experimental import pallas as pl
from jax.experimental.pallas import tpu as pltpu
from jax.sharding import PartitionSpec as P

LANES = 128
PAD = 8
PLANES = 4
BLOCK = 2048
MESH = pl.DeviceIdType.MESH


def join_kernel(
    cfg,
    owner_hbm, lane_hbm, offset_hbm, age_hbm, size_hbm, rates_hbm, quotes_ref, quotes_flat,
    out_ref,
    owner_v, lane_v, offset_v, age_v, size_v, rates_v,
    table, recv, sbuf, msg_row, msg_age, got_row, got_age, key_v, scale_v, cur, prev, bsend, brecv, tail,
    isem, qsem, bsem, rsend, rrecv, arecv, jsend, jrecv, relay,
):
    tm_n, sym_n, cap = cfg
    devices = tm_n * sym_n
    ticks = owner_v.shape[1]
    lane_count, quote_rows, features = quotes_ref.shape
    stride = quote_rows + PAD
    tm, sym = lax.axis_index("tm"), lax.axis_index("sym")
    me = tm * sym_n + sym

    plane_n = devices // PLANES
    bits = plane_n.bit_length() - 1
    z = lax.div(me, plane_n)
    half, quarter = lax.div(z, 2), lax.rem(z, 2)
    inner = lax.rem(half + quarter, 2)
    here = lax.rem(me, plane_n)

    def device(p):
        return (lax.div(p, sym_n), lax.rem(p, sym_n))

    flip = [(1 << i) - (2 << i) * lax.rem(lax.div(here, 1 << i), 2) for i in range(bits)]

    def mate(j):
        q = here
        for i, step in enumerate(flip):
            if not isinstance(j, int):
                q = q + lax.rem(lax.div(j, 1 << i), 2) * step
            elif j >> i & 1:
                q = q + step
        return q

    other = 1 - half
    plane = [z, 2 * half + 1 - quarter, 2 * other + half, 2 * other + other]

    def pick(outer_g, inner_g):
        return plane[outer_g] + inner * (plane[inner_g] - plane[outer_g])

    small = [
        pltpu.make_async_copy(src, dst, isem.at[i])
        for i, (src, dst) in enumerate([
            (owner_hbm, owner_v), (lane_hbm, lane_v), (offset_hbm, offset_v), (age_hbm, age_v),
            (rates_hbm, rates_v), (size_hbm, size_v),
        ])
    ]
    last_rows = pltpu.make_async_copy(
        quotes_ref.at[:, pl.ds(quote_rows - PAD, PAD)], tail, isem.at[6]
    )
    for copy in small:
        copy.start()
    last_rows.start()

    barrier = pltpu.get_barrier_semaphore()

    def greet(p):
        pl.semaphore_signal(barrier, inc=1, device_id=device(p), device_id_type=MESH)

    rows_n = tm_n // PLANES
    first_row = 1 - lax.div(lax.rem(tm, rows_n) + rows_n - 1, rows_n)
    last_row = lax.div(lax.rem(tm, rows_n) + 1, rows_n)

    @pl.when(inner == 1)
    def _():
        for j in range(plane_n):
            greet(plane[2] * plane_n + mate(j))
        for j in range(plane_n):
            greet(plane[1] * plane_n + mate(j))

    @pl.when(inner == 0)
    def _():
        greet(plane[1] * plane_n + here)

    for j in range(plane_n - 1, 0, -1):
        greet(z * plane_n + mate(j))

    loads = [
        pltpu.make_async_copy(
            quotes_ref.at[lane], table.at[pl.ds(lane * stride + PAD, quote_rows)], qsem
        )
        for lane in range(lane_count)
    ]
    for load in loads:
        load.start()
    for copy in small:
        copy.wait()

    owner = owner_v[...]
    mine = owner == lax.broadcasted_iota(jnp.int32, (devices, ticks), 0)
    hot = mine.astype(jnp.float32)
    hot_b = hot.astype(jnp.bfloat16)
    width = 256 if ticks % 256 == 0 else 128
    upper = (
        lax.broadcasted_iota(jnp.int32, (width, width), 0)
        < lax.broadcasted_iota(jnp.int32, (width, width), 1)
    ).astype(jnp.float32).astype(jnp.bfloat16)
    base = jnp.zeros((devices, 1), jnp.float32)
    ranks = []
    for start in range(0, ticks, width):
        part = hot[:, start:start + width]
        before = jnp.dot(
            hot_b[:, start:start + width], upper, preferred_element_type=jnp.float32
        )
        ranks.append(jnp.sum(part * (before + base), axis=0, keepdims=True))
        base = base + jnp.sum(part, axis=1, keepdims=True)
    rank = jnp.concatenate(ranks, axis=1).astype(jnp.int32)
    key = owner * LANES + jnp.clip(rank, 0, cap - 1)

    place = (
        rank == lax.broadcasted_iota(jnp.int32, (LANES, ticks), 0)
    ).astype(jnp.float32).astype(jnp.bfloat16)
    local = lane_v[...] * stride + PAD - 1 + offset_v[...]
    age = age_v[...]
    high = age.astype(jnp.bfloat16).astype(jnp.float32)
    middle = (age - high).astype(jnp.bfloat16).astype(jnp.float32)
    low = age - high - middle
    pieces = [
        (local // LANES).astype(jnp.float32), (local % LANES).astype(jnp.float32), high, middle, low
    ]
    spread = jnp.concatenate([(hot * piece).astype(jnp.bfloat16) for piece in pieces], axis=0)
    put = lax.dot_general(
        spread, place, (((1,), (1,)), ((), ())), preferred_element_type=jnp.float32
    )
    taken = [put[i * devices:(i + 1) * devices] for i in range(5)]
    msg_row[:, 0, :] = jnp.clip(
        (taken[0] * LANES + taken[1]).astype(jnp.int32), PAD - 1, lane_count * stride - 2
    )
    msg_age[:, 0, :] = (taken[2] + taken[3]) + taken[4]

    def row_message(p, slot):
        return pltpu.make_async_remote_copy(
            src_ref=msg_row.at[p], dst_ref=got_row.at[slot],
            send_sem=rsend, recv_sem=rrecv.at[slot],
            device_id=device(p), device_id_type=MESH,
        )

    def age_message(p, slot):
        return pltpu.make_async_remote_copy(
            src_ref=msg_age.at[p], dst_ref=got_age.at[slot],
            send_sem=rsend, recv_sem=arecv.at[slot],
            device_id=device(p), device_id_type=MESH,
        )

    def ask(where, first, last):
        for j in range(first, last):
            p = where * plane_n + mate(j)
            row_message(p, me).start()
            age_message(p, me).start()

    def boundary():
        return pltpu.make_async_remote_copy(
            src_ref=bsend, dst_ref=brecv, send_sem=bsem.at[0], recv_sem=bsem.at[1],
            device_id=(lax.rem(tm + 1, tm_n), sym), device_id_type=MESH,
        )

    last_rows.wait()
    for lane in range(lane_count):
        bsend[lane:lane + 1, :] = tail[lane, PAD - 1:PAD, :]

    def tell(where, which):
        pl.semaphore_signal(
            relay.at[which], inc=1, device_id=device(where * plane_n + here), device_id_type=MESH
        )

    def heard(which):
        pl.semaphore_wait(relay.at[which], 1)

    near = pick(1, 2)

    pl.semaphore_wait(barrier, 2 * plane_n - 1 + inner)

    @pl.when(last_row * half == 0)
    def _():
        boundary().start()

    ask(near, 0, plane_n)

    @pl.when(inner == 1)
    def _():
        tell(plane[1], 1)
        heard(1)
        tell(plane[2], 2)

        @pl.when(last_row * half == 1)
        def _():
            boundary().start()

        ask(plane[1], 0, plane_n)
        heard(2)
        tell(plane[1], 2)
        ask(plane[3], 0, plane_n)

    @pl.when(inner == 0)
    def _():
        tell(plane[1], 1)
        heard(1)
        ask(plane[2], 0, plane_n)
        heard(2)
        ask(plane[3], 0, plane_n)

    ask(z, 1, plane_n)

    own_row = pltpu.make_async_copy(msg_row.at[me], got_row.at[me], isem.at[0])
    own_row.start()

    @pl.when(tm == 0)
    def _():
        brecv[...] = jnp.zeros_like(brecv)

    @pl.when(tm > 0)
    def _():
        boundary().wait_recv()

    pltpu.make_async_copy(
        quotes_flat, table.at[pl.ds(0, lane_count * quote_rows)], qsem
    ).wait()
    edge = brecv[...]
    for lane in range(lane_count):
        table[lane * stride + PAD - 1:lane * stride + PAD, :] = edge[lane:lane + 1, :]

    rates = rates_v[...]

    def joined(p, ages):
        for r in range(cap):
            row = got_row[p, 0, r]
            cur[r:r + 1, :] = table[pl.ds(row + 1, 1), :]
            prev[r:r + 1, :] = table[pl.ds(row, 1), :]
        ages = jnp.transpose(jnp.broadcast_to(ages, (LANES, LANES)))[:cap]
        weight = jnp.exp(-ages * rates)
        return weight * cur[...] + (1.0 - weight) * prev[...]

    def share(p, source):
        return pltpu.make_async_remote_copy(
            src_ref=sbuf.at[p], dst_ref=recv.at[source, pl.ds(0, cap)],
            send_sem=jsend, recv_sem=jrecv.at[lax.div(source, 2)],
            device_id=device(p), device_id_type=MESH,
        )

    def sent(src, dst, sem):
        pltpu.make_async_remote_copy(
            src_ref=src.at[pl.ds(0, devices - 1)], dst_ref=dst, send_sem=sem,
            recv_sem=jrecv.at[0], device_id=device(z * plane_n + mate(1)), device_id_type=MESH,
        ).wait_send()

    def serve(where, first, last):
        @pl.loop(first, last)
        def _(j):
            p = where * plane_n + mate(j)
            row_message(p, p).wait_recv()
            age_message(p, p).wait_recv()
            sbuf[p] = joined(p, got_age[p])
            share(p, me).start()

    few = plane_n // 4
    serve(pick(1, 2), 0, few)
    serve(pick(2, 3), 0, plane_n)
    serve(pick(1, 2), few, plane_n)
    serve(pick(3, 1), 0, plane_n)
    serve(z, 1, plane_n)

    @pl.when(tm < tm_n - 1)
    def _():
        boundary().wait_send()

    sent(msg_age, got_age.at[pl.ds(0, devices - 1)], rsend)
    sent(msg_age, got_age.at[pl.ds(0, devices - 1)], rsend)
    own_row.wait()
    recv[me, 0:cap, :] = joined(me, msg_age[me])
    if cap < LANES:
        @pl.loop(0, devices)
        def _(p):
            recv[p, cap:, :] = jnp.zeros((LANES - cap, features), jnp.float32)

    for start in range(0, ticks, LANES):
        key_v[start:start + LANES, :] = jnp.transpose(
            jnp.broadcast_to(key[:, start:start + LANES], (LANES, LANES))
        )
        scale_v[start:start + LANES, :] = jnp.transpose(
            jnp.broadcast_to(size_v[:, start:start + LANES], (LANES, LANES))
        )

    block = BLOCK if ticks % BLOCK == 0 else LANES
    slots = lax.broadcasted_iota(jnp.int32, (1, LANES), 1)

    def absorb(pa, pb, fresh=False, final=False):
        both = jnp.concatenate([recv[pa], recv[pb]], axis=0)
        first = both.astype(jnp.bfloat16)
        second = (both - first.astype(jnp.float32)).astype(jnp.bfloat16)
        parts = jnp.concatenate([first, second], axis=1)
        slot_a, slot_b = pa * LANES + slots, pb * LANES + slots

        @pl.loop(0, ticks // block)
        def _(b):
            rows = pl.ds(pl.multiple_of(b * block, block), block)
            keys = key_v[rows, :]
            chosen = jnp.concatenate([
                (keys == slot_a).astype(jnp.float32).astype(jnp.bfloat16),
                (keys == slot_b).astype(jnp.float32).astype(jnp.bfloat16),
            ], axis=1)
            got = jnp.dot(chosen, parts, preferred_element_type=jnp.float32)
            got = got[:, :features] + got[:, features:]
            if not fresh:
                got = out_ref[rows, :] + got
            out_ref[rows, :] = got * scale_v[rows, :] if final else got

    def both_shares(pair):
        two = pl.ds(2 * pair, 2)
        return pltpu.make_async_remote_copy(
            src_ref=sbuf.at[two], dst_ref=recv.at[two, pl.ds(0, cap)],
            send_sem=jsend, recv_sem=jrecv.at[pair],
            device_id=device(2 * pair), device_id_type=MESH,
        )

    partner = z * plane_n + mate(1)
    share(partner, partner).wait_recv()
    absorb(me, partner, fresh=True)

    def collect(where, i, final=False):
        pa = where * plane_n + mate(2 * i)
        pb = where * plane_n + mate(2 * i + 1)
        both_shares(lax.div(pa, 2)).wait_recv()
        absorb(pa, pb, final=final)

    pairs = plane_n // 2
    last = pick(3, 2)
    for where, first, stop in (
        (z, 1, pairs), (plane[1], 0, pairs), (pick(2, 3), 0, pairs), (last, 0, pairs - 1),
    ):
        @pl.loop(first, stop)
        def _(i, where=where):
            collect(where, i)

    collect(last, pairs - 1, True)

    sent(sbuf, recv.at[pl.ds(0, devices - 1), pl.ds(0, cap)], jsend)


def per_device(trade_age, trade_size, owner, symbol_lane, quote_offset, quotes, rates):
    tm_n, sym_n = lax.axis_size("tm"), lax.axis_size("sym")
    devices = tm_n * sym_n
    ticks = trade_age.shape[0]
    cap = 3 * ticks // (2 * devices)
    lane_count, quote_rows, features = quotes.shape
    dma = pltpu.SemaphoreType.DMA
    operands = [
        pltpu.with_memory_space_constraint(x, pltpu.HBM)
        for x in (
            owner.reshape(1, ticks), symbol_lane.reshape(1, ticks),
            quote_offset.reshape(1, ticks), trade_age.reshape(1, ticks),
            trade_size.reshape(1, ticks),
            rates.reshape(1, features), quotes, quotes.reshape(-1, features),
        )
    ]
    joined = pl.pallas_call(
        functools.partial(join_kernel, (tm_n, sym_n, cap)),
        out_shape=jax.ShapeDtypeStruct((ticks, features), jnp.float32),
        in_specs=[pl.BlockSpec(memory_space=pltpu.HBM)] * 8,
        out_specs=pl.BlockSpec(memory_space=pltpu.VMEM),
        scratch_shapes=[
            pltpu.VMEM((1, ticks), jnp.int32),
            pltpu.VMEM((1, ticks), jnp.int32),
            pltpu.VMEM((1, ticks), jnp.int32),
            pltpu.VMEM((1, ticks), jnp.float32),
            pltpu.VMEM((1, ticks), jnp.float32),
            pltpu.VMEM((1, features), jnp.float32),
            pltpu.VMEM((lane_count * (quote_rows + PAD), features), jnp.float32),
            pltpu.VMEM((devices, LANES, features), jnp.float32),
            pltpu.VMEM((devices, cap, features), jnp.float32),
            pltpu.VMEM((devices, 1, LANES), jnp.int32),
            pltpu.VMEM((devices, 1, LANES), jnp.float32),
            pltpu.SMEM((devices, 1, LANES), jnp.int32),
            pltpu.VMEM((devices, 1, LANES), jnp.float32),
            pltpu.VMEM((ticks, LANES), jnp.int32),
            pltpu.VMEM((ticks, features), jnp.float32),
            pltpu.VMEM((cap, features), jnp.float32),
            pltpu.VMEM((cap, features), jnp.float32),
            pltpu.VMEM((lane_count, features), jnp.float32),
            pltpu.VMEM((lane_count, features), jnp.float32),
            pltpu.VMEM((lane_count, PAD, features), jnp.float32),
            dma((7,)), dma, dma((2,)),
            dma, dma((devices,)), dma((devices,)), dma, dma((devices // 2,)),
            pltpu.SemaphoreType.REGULAR((3,)),
        ],
        compiler_params=pltpu.CompilerParams(
            collective_id=0, has_side_effects=True, vmem_limit_bytes=32 << 20
        ),
    )(*operands)
    return joined


def solution(mesh):
    in_specs = (
        P(("tm", "sym")),
        P(("tm", "sym")),
        P(("tm", "sym"), None),
        P(("tm", "sym")),
        P(("tm", "sym")),
        P("sym", "tm", None),
        P(),
    )
    out_specs = P(("tm", "sym"), None)
    return jax.shard_map(
        per_device, mesh=mesh, in_specs=in_specs, out_specs=out_specs, check_vma=False
    )
```

```python
import functools

import jax
import jax.numpy as jnp
from jax import lax
from jax.experimental import pallas as pl
from jax.experimental.pallas import tpu as pltpu
from jax.sharding import PartitionSpec as P

LANES = 128
PAD = 8
PLANES = 4
BLOCK = 2048
STORES = 4
MESH = pl.DeviceIdType.MESH


def join_kernel(
    cfg,
    owner_hbm, lane_hbm, offset_hbm, age_hbm, size_hbm, rates_hbm, quotes_ref, quotes_flat,
    out_ref, pair_ref, place_v, scale_v,
    owner_v, lane_v, offset_v, age_v, size_v, rates_v,
    table, recv, sbuf, msg_row, msg_age, got_row, got_age, key_v, cur, prev, bsend, brecv, tail,
    isem, qsem, bsem, rsend, rrecv, arecv, jsend, jrecv, relay,
):
    tm_n, sym_n, cap = cfg
    devices = tm_n * sym_n
    ticks = owner_v.shape[1]
    lane_count, quote_rows, features = quotes_ref.shape
    stride = quote_rows + PAD
    tm, sym = lax.axis_index("tm"), lax.axis_index("sym")
    me = tm * sym_n + sym

    plane_n = devices // PLANES
    bits = plane_n.bit_length() - 1
    z = lax.div(me, plane_n)
    half, quarter = lax.div(z, 2), lax.rem(z, 2)
    inner = lax.rem(half + quarter, 2)
    here = lax.rem(me, plane_n)

    def device(p):
        return (lax.div(p, sym_n), lax.rem(p, sym_n))

    flip = [(1 << i) - (2 << i) * lax.rem(lax.div(here, 1 << i), 2) for i in range(bits)]

    def mate(j):
        q = here
        for i, step in enumerate(flip):
            if not isinstance(j, int):
                q = q + lax.rem(lax.div(j, 1 << i), 2) * step
            elif j >> i & 1:
                q = q + step
        return q

    other = 1 - half
    plane = [z, 2 * half + 1 - quarter, 2 * other + half, 2 * other + other]

    def pick(outer_g, inner_g):
        return plane[outer_g] + inner * (plane[inner_g] - plane[outer_g])

    small = [
        pltpu.make_async_copy(src, dst, isem.at[i])
        for i, (src, dst) in enumerate([
            (owner_hbm, owner_v), (lane_hbm, lane_v), (offset_hbm, offset_v), (age_hbm, age_v),
            (rates_hbm, rates_v), (size_hbm, size_v),
        ])
    ]
    last_rows = pltpu.make_async_copy(
        quotes_ref.at[:, pl.ds(quote_rows - PAD, PAD)], tail, isem.at[6]
    )
    for copy in small:
        copy.start()
    last_rows.start()

    barrier = pltpu.get_barrier_semaphore()

    def greet(p):
        pl.semaphore_signal(barrier, inc=1, device_id=device(p), device_id_type=MESH)

    rows_n = tm_n // PLANES
    first_row = 1 - lax.div(lax.rem(tm, rows_n) + rows_n - 1, rows_n)
    last_row = lax.div(lax.rem(tm, rows_n) + 1, rows_n)

    @pl.when(inner == 1)
    def _():
        for j in range(plane_n):
            greet(plane[2] * plane_n + mate(j))
        for j in range(plane_n):
            greet(plane[1] * plane_n + mate(j))

    @pl.when(inner == 0)
    def _():
        greet(plane[1] * plane_n + here)

    for j in range(plane_n - 1, 0, -1):
        greet(z * plane_n + mate(j))

    loads = [
        pltpu.make_async_copy(
            quotes_ref.at[lane], table.at[pl.ds(lane * stride + PAD, quote_rows)], qsem
        )
        for lane in range(lane_count)
    ]
    for load in loads:
        load.start()
    for copy in small:
        copy.wait()

    owner = owner_v[...]
    mine = owner == lax.broadcasted_iota(jnp.int32, (devices, ticks), 0)
    hot = mine.astype(jnp.float32)
    hot_b = hot.astype(jnp.bfloat16)
    width = 256 if ticks % 256 == 0 else 128
    upper = (
        lax.broadcasted_iota(jnp.int32, (width, width), 0)
        < lax.broadcasted_iota(jnp.int32, (width, width), 1)
    ).astype(jnp.float32).astype(jnp.bfloat16)
    base = jnp.zeros((devices, 1), jnp.float32)
    ranks = []
    for start in range(0, ticks, width):
        part = hot[:, start:start + width]
        before = jnp.dot(
            hot_b[:, start:start + width], upper, preferred_element_type=jnp.float32
        )
        ranks.append(jnp.sum(part * (before + base), axis=0, keepdims=True))
        base = base + jnp.sum(part, axis=1, keepdims=True)
    rank = jnp.concatenate(ranks, axis=1).astype(jnp.int32)
    key = owner * LANES + jnp.clip(rank, 0, cap - 1)

    place = (
        rank == lax.broadcasted_iota(jnp.int32, (LANES, ticks), 0)
    ).astype(jnp.float32).astype(jnp.bfloat16)
    local = lane_v[...] * stride + PAD - 1 + offset_v[...]
    age = age_v[...]
    high = age.astype(jnp.bfloat16).astype(jnp.float32)
    middle = (age - high).astype(jnp.bfloat16).astype(jnp.float32)
    low = age - high - middle
    pieces = [
        (local // LANES).astype(jnp.float32), (local % LANES).astype(jnp.float32), high, middle, low
    ]
    spread = jnp.concatenate([(hot * piece).astype(jnp.bfloat16) for piece in pieces], axis=0)
    put = lax.dot_general(
        spread, place, (((1,), (1,)), ((), ())), preferred_element_type=jnp.float32
    )
    taken = [put[i * devices:(i + 1) * devices] for i in range(5)]
    msg_row[:, 0, :] = jnp.clip(
        (taken[0] * LANES + taken[1]).astype(jnp.int32), PAD - 1, lane_count * stride - 2
    )
    msg_age[:, 0, :] = (taken[2] + taken[3]) + taken[4]

    def row_message(p, slot):
        return pltpu.make_async_remote_copy(
            src_ref=msg_row.at[p], dst_ref=got_row.at[slot],
            send_sem=rsend, recv_sem=rrecv.at[slot],
            device_id=device(p), device_id_type=MESH,
        )

    def age_message(p, slot):
        return pltpu.make_async_remote_copy(
            src_ref=msg_age.at[p], dst_ref=got_age.at[slot],
            send_sem=rsend, recv_sem=arecv.at[slot],
            device_id=device(p), device_id_type=MESH,
        )

    def ask(where, first, last):
        for j in range(first, last):
            p = where * plane_n + mate(j)
            row_message(p, me).start()
            age_message(p, me).start()

    def boundary():
        return pltpu.make_async_remote_copy(
            src_ref=bsend, dst_ref=brecv, send_sem=bsem.at[0], recv_sem=bsem.at[1],
            device_id=(lax.rem(tm + 1, tm_n), sym), device_id_type=MESH,
        )

    last_rows.wait()
    for lane in range(lane_count):
        bsend[lane:lane + 1, :] = tail[lane, PAD - 1:PAD, :]

    def tell(where, which):
        pl.semaphore_signal(
            relay.at[which], inc=1, device_id=device(where * plane_n + here), device_id_type=MESH
        )

    def heard(which):
        pl.semaphore_wait(relay.at[which], 1)

    near = pick(1, 2)

    pl.semaphore_wait(barrier, 2 * plane_n - 1 + inner)

    @pl.when(last_row * half == 0)
    def _():
        boundary().start()

    ask(near, 0, plane_n)

    @pl.when(inner == 1)
    def _():
        tell(plane[1], 1)
        heard(1)
        tell(plane[2], 2)

        @pl.when(last_row * half == 1)
        def _():
            boundary().start()

        ask(plane[1], 0, plane_n)
        heard(2)
        tell(plane[1], 2)
        ask(plane[3], 0, plane_n)

    @pl.when(inner == 0)
    def _():
        tell(plane[1], 1)
        heard(1)
        ask(plane[2], 0, plane_n)
        heard(2)
        ask(plane[3], 0, plane_n)

    ask(z, 1, plane_n)

    own_row = pltpu.make_async_copy(msg_row.at[me], got_row.at[me], isem.at[0])
    own_row.start()

    @pl.when(tm == 0)
    def _():
        brecv[...] = jnp.zeros_like(brecv)

    @pl.when(tm > 0)
    def _():
        boundary().wait_recv()

    pltpu.make_async_copy(
        quotes_flat, table.at[pl.ds(0, lane_count * quote_rows)], qsem
    ).wait()
    edge = brecv[...]
    for lane in range(lane_count):
        table[lane * stride + PAD - 1:lane * stride + PAD, :] = edge[lane:lane + 1, :]

    rates = rates_v[...]

    def joined(p, ages):
        for r in range(cap):
            row = got_row[p, 0, r]
            cur[r:r + 1, :] = table[pl.ds(row + 1, 1), :]
            prev[r:r + 1, :] = table[pl.ds(row, 1), :]
        ages = jnp.transpose(jnp.broadcast_to(ages, (LANES, LANES)))[:cap]
        weight = jnp.exp(-ages * rates)
        return weight * cur[...] + (1.0 - weight) * prev[...]

    def share(p, source):
        return pltpu.make_async_remote_copy(
            src_ref=sbuf.at[p], dst_ref=recv.at[source, pl.ds(0, cap)],
            send_sem=jsend, recv_sem=jrecv.at[lax.div(source, 2)],
            device_id=device(p), device_id_type=MESH,
        )

    def sent(src, dst, sem):
        pltpu.make_async_remote_copy(
            src_ref=src.at[pl.ds(0, devices - 1)], dst_ref=dst, send_sem=sem,
            recv_sem=jrecv.at[0], device_id=device(z * plane_n + mate(1)), device_id_type=MESH,
        ).wait_send()

    def serve(where, first, last):
        @pl.loop(first, last)
        def _(j):
            p = where * plane_n + mate(j)
            row_message(p, p).wait_recv()
            age_message(p, p).wait_recv()
            sbuf[p] = joined(p, got_age[p])
            share(p, me).start()

    few = plane_n // 4
    serve(pick(1, 2), 0, few)
    serve(pick(2, 3), 0, plane_n)
    serve(pick(1, 2), few, plane_n)
    serve(pick(3, 1), 0, plane_n)
    serve(z, 1, plane_n)

    @pl.when(tm < tm_n - 1)
    def _():
        boundary().wait_send()

    sent(msg_age, got_age.at[pl.ds(0, devices - 1)], rsend)
    sent(msg_age, got_age.at[pl.ds(0, devices - 1)], rsend)
    own_row.wait()
    recv[me, 0:cap, :] = joined(me, msg_age[me])
    if cap < LANES:
        @pl.loop(0, devices)
        def _(p):
            recv[p, cap:, :] = jnp.zeros((LANES - cap, features), jnp.float32)

    pairs = plane_n // 2
    last = pick(3, 2)
    chip = lax.div(last * plane_n + mate(plane_n - 1), 2)
    for start in range(0, ticks, LANES):
        key_v[start:start + LANES, :] = jnp.transpose(
            jnp.broadcast_to(key[:, start:start + LANES], (LANES, LANES))
        )
        place_v[start:start + LANES, :] = key_v[start:start + LANES, :] - chip * (2 * LANES)
        scale_v[start:start + LANES, :] = jnp.transpose(
            jnp.broadcast_to(size_v[:, start:start + LANES], (LANES, LANES))
        )

    block = BLOCK if ticks % BLOCK == 0 else LANES
    slots = lax.broadcasted_iota(jnp.int32, (1, LANES), 1)

    def absorb(pa, pb, fresh=False):
        both = jnp.concatenate([recv[pa], recv[pb]], axis=0)
        first = both.astype(jnp.bfloat16)
        second = (both - first.astype(jnp.float32)).astype(jnp.bfloat16)
        parts = jnp.concatenate([first, second], axis=1)
        slot_a, slot_b = pa * LANES + slots, pb * LANES + slots

        @pl.loop(0, ticks // block)
        def _(b):
            rows = pl.ds(pl.multiple_of(b * block, block), block)
            keys = key_v[rows, :]
            chosen = jnp.concatenate([
                (keys == slot_a).astype(jnp.float32).astype(jnp.bfloat16),
                (keys == slot_b).astype(jnp.float32).astype(jnp.bfloat16),
            ], axis=1)
            got = jnp.dot(chosen, parts, preferred_element_type=jnp.float32)
            got = got[:, :features] + got[:, features:]
            if not fresh:
                got = out_ref[rows, :] + got
            out_ref[rows, :] = got

    def both_shares(pair):
        two = pl.ds(2 * pair, 2)
        return pltpu.make_async_remote_copy(
            src_ref=sbuf.at[two], dst_ref=recv.at[two, pl.ds(0, cap)],
            send_sem=jsend, recv_sem=jrecv.at[pair],
            device_id=device(2 * pair), device_id_type=MESH,
        )

    partner = z * plane_n + mate(1)
    share(partner, partner).wait_recv()
    absorb(me, partner, fresh=True)

    def collect(where, i):
        pa = where * plane_n + mate(2 * i)
        pb = where * plane_n + mate(2 * i + 1)
        both_shares(lax.div(pa, 2)).wait_recv()
        absorb(pa, pb)

    for where, first, stop in (
        (z, 1, pairs), (plane[1], 0, pairs), (pick(2, 3), 0, pairs), (last, 0, pairs - 1),
    ):
        @pl.loop(first, stop)
        def _(i, where=where):
            collect(where, i)

    both_shares(chip).wait_recv()
    pair_ref[0:LANES, :] = recv[2 * chip]
    pair_ref[LANES:, :] = recv[2 * chip + 1]

    sent(sbuf, recv.at[pl.ds(0, devices - 1), pl.ds(0, cap)], jsend)


def store_kernel(joined_ref, pair_ref, place_ref, scale_ref, out_ref, done_v, sem):
    ticks, features = joined_ref.shape
    block = ticks // STORES
    both = pair_ref[...]
    first = both.astype(jnp.bfloat16)
    second = (both - first.astype(jnp.float32)).astype(jnp.bfloat16)
    parts = jnp.concatenate([first, second], axis=1)
    slots = lax.broadcasted_iota(jnp.int32, (1, LANES), 1)
    copies = []
    for i in range(STORES):
        rows = pl.ds(i * block, block)
        place = place_ref[rows, :]
        chosen = jnp.concatenate([
            (place == slots).astype(jnp.float32).astype(jnp.bfloat16),
            (place == slots + LANES).astype(jnp.float32).astype(jnp.bfloat16),
        ], axis=1)
        got = jnp.dot(chosen, parts, preferred_element_type=jnp.float32)
        got = joined_ref[rows, :] + (got[:, :features] + got[:, features:])
        done_v[rows, :] = got * scale_ref[rows, :]
        copies.append(pltpu.make_async_copy(done_v.at[rows], out_ref.at[rows], sem.at[i]))
        copies[-1].start()
    for copy in copies:
        copy.wait()


def per_device(trade_age, trade_size, owner, symbol_lane, quote_offset, quotes, rates):
    tm_n, sym_n = lax.axis_size("tm"), lax.axis_size("sym")
    devices = tm_n * sym_n
    ticks = trade_age.shape[0]
    cap = 3 * ticks // (2 * devices)
    lane_count, quote_rows, features = quotes.shape
    dma = pltpu.SemaphoreType.DMA
    operands = [
        pltpu.with_memory_space_constraint(x, pltpu.HBM)
        for x in (
            owner.reshape(1, ticks), symbol_lane.reshape(1, ticks),
            quote_offset.reshape(1, ticks), trade_age.reshape(1, ticks),
            trade_size.reshape(1, ticks),
            rates.reshape(1, features), quotes, quotes.reshape(-1, features),
        )
    ]
    parts = pl.pallas_call(
        functools.partial(join_kernel, (tm_n, sym_n, cap)),
        out_shape=[
            jax.ShapeDtypeStruct((ticks, features), jnp.float32),
            jax.ShapeDtypeStruct((2 * LANES, features), jnp.float32),
            jax.ShapeDtypeStruct((ticks, LANES), jnp.int32),
            jax.ShapeDtypeStruct((ticks, features), jnp.float32),
        ],
        in_specs=[pl.BlockSpec(memory_space=pltpu.HBM)] * 8,
        out_specs=[pl.BlockSpec(memory_space=pltpu.VMEM)] * 4,
        scratch_shapes=[
            pltpu.VMEM((1, ticks), jnp.int32),
            pltpu.VMEM((1, ticks), jnp.int32),
            pltpu.VMEM((1, ticks), jnp.int32),
            pltpu.VMEM((1, ticks), jnp.float32),
            pltpu.VMEM((1, ticks), jnp.float32),
            pltpu.VMEM((1, features), jnp.float32),
            pltpu.VMEM((lane_count * (quote_rows + PAD), features), jnp.float32),
            pltpu.VMEM((devices, LANES, features), jnp.float32),
            pltpu.VMEM((devices, cap, features), jnp.float32),
            pltpu.VMEM((devices, 1, LANES), jnp.int32),
            pltpu.VMEM((devices, 1, LANES), jnp.float32),
            pltpu.SMEM((devices, 1, LANES), jnp.int32),
            pltpu.VMEM((devices, 1, LANES), jnp.float32),
            pltpu.VMEM((ticks, LANES), jnp.int32),
            pltpu.VMEM((cap, features), jnp.float32),
            pltpu.VMEM((cap, features), jnp.float32),
            pltpu.VMEM((lane_count, features), jnp.float32),
            pltpu.VMEM((lane_count, features), jnp.float32),
            pltpu.VMEM((lane_count, PAD, features), jnp.float32),
            dma((7,)), dma, dma((2,)),
            dma, dma((devices,)), dma((devices,)), dma, dma((devices // 2,)),
            pltpu.SemaphoreType.REGULAR((3,)),
        ],
        compiler_params=pltpu.CompilerParams(
            collective_id=0, has_side_effects=True, vmem_limit_bytes=32 << 20
        ),
    )(*operands)
    return pl.pallas_call(
        store_kernel,
        out_shape=jax.ShapeDtypeStruct((ticks, features), jnp.float32),
        in_specs=[pl.BlockSpec(memory_space=pltpu.VMEM)] * 4,
        out_specs=pl.BlockSpec(memory_space=pltpu.HBM),
        scratch_shapes=[pltpu.VMEM((ticks, features), jnp.float32), dma((STORES,))],
        compiler_params=pltpu.CompilerParams(vmem_limit_bytes=16 << 20),
    )(*parts)


def solution(mesh):
    in_specs = (
        P(("tm", "sym")),
        P(("tm", "sym")),
        P(("tm", "sym"), None),
        P(("tm", "sym")),
        P(("tm", "sym")),
        P("sym", "tm", None),
        P(),
    )
    out_specs = P(("tm", "sym"), None)
    return jax.shard_map(
        per_device, mesh=mesh, in_specs=in_specs, out_specs=out_specs, check_vma=False
    )
```
